32 devices in a mesh: section: 2 (over x), dp: 16 (over z, y, core).
Axes of the slice: x: 2, y: 2, z: 4, core: 2. Of those that a mesh axis runs over, the one named last changes fastest.
Arguments:
- teacher_hidden: bfloat16 [64, 8192], P('dp'), may hold values from -12 to 12
- student_hidden: bfloat16 [64, 3584], P('dp'), may hold values from -12 to 12
- teacher_gain: bfloat16 [8192], replicated, may hold values from 0.5 to 1.5
- student_gain: bfloat16 [3584], replicated, may hold values from 0.5 to 1.5
- teacher_head: bfloat16 [5120, 8192], P(('section', 'dp')), may hold values from -64 to 64
- student_head: bfloat16 [5120, 3584], P(('section', 'dp')), may hold values from -64 to 64
- labels: int32 [64], replicated, may hold values from 0 to 5119
- cotangent: float32 [64], replicated, may hold values from 2 to 20
Outputs:
- loss: float32 [], replicated
- student_grad: float32 [64, 3584], P('dp')
- gain_grad: float32 [3584], replicated
- head_grad: bfloat16 [5120, 3584], P(('section', 'dp'))
The draws below stay inside these ranges and needn't reach their ends.
All inputs are finite; a program needn't handle non-finite values.
Results may differ from the reference program's by a relative error of at most 0.0079.
Values may be sent and summed in bfloat16 or wider, within the bound.
A program may use at most 64 MiB of HBM per device.

```python
import math
import jax
import jax.numpy as jnp
from jax import lax

DT = 8192
DS = 3584
TOKENS = 64
VOCAB = 5120


def unit_column(head_key, index, width):
    return jnp.clip(jax.random.normal(jax.random.fold_in(head_key, index), (width,), jnp.float32), -5.0, 5.0)


def chosen_rows(pick_key):
    return jax.random.randint(pick_key, (8, 2), 0, VOCAB)


def head_block(head_key, width, pick_key):
    rows = jax.vmap(lambda index: unit_column(head_key, index, width))(jnp.arange(VOCAB))
    boost = max(1.0, 90.0 / float(width) ** 0.5)
    picks = chosen_rows(pick_key).reshape(-1)
    marked = jnp.any(jnp.arange(VOCAB)[:, None] == picks[None, :], axis=1)
    factor = jnp.where(marked, boost, 1.0).astype(jnp.float32)[:, None]
    return rows * factor * (4.0 / jnp.sqrt(jnp.float32(width)))


def aligned_hidden(noise_key, width, head_key, pick_key):
    base = jnp.clip(jax.random.normal(noise_key, (TOKENS, width), jnp.float32), -6.0, 6.0)
    picks = chosen_rows(pick_key)
    first = jax.vmap(lambda index: unit_column(head_key, index, width))(picks[:, 0])
    second = jax.vmap(lambda index: unit_column(head_key, index, width))(picks[:, 1])
    strength = jnp.array([1.0, 0.9, 0.8, 0.7, 1.0, 0.9, 0.8, 0.7], jnp.float32)[:, None]
    rows = strength * (first + 0.99 * second) / 1.41 + jnp.sqrt(1.0 - strength * strength) * base[-8:]
    base = base.at[-8:].set(rows)
    return jnp.clip(base, -12.0, 12.0)


def draw_teacher_head(key, part):
    return head_block(jax.random.fold_in(key, 101), DT, jax.random.fold_in(key, 303)).astype(jnp.bfloat16)


def draw_student_head(key, part):
    return head_block(jax.random.fold_in(key, 202), DS, jax.random.fold_in(key, 404)).astype(jnp.bfloat16)


def draw_teacher_hidden(key, part):
    return aligned_hidden(jax.random.fold_in(key, 11), DT, jax.random.fold_in(key, 101), jax.random.fold_in(key, 303)).astype(jnp.bfloat16)


def draw_student_hidden(key, part):
    return aligned_hidden(jax.random.fold_in(key, 12), DS, jax.random.fold_in(key, 202), jax.random.fold_in(key, 404)).astype(jnp.bfloat16)


def place_ends(drawn, key, low, top_value):
    index_at = [jax.random.randint(jax.random.fold_in(key, axis), (), 0, length) for axis, length in enumerate(drawn.shape)]
    longest = drawn.shape.index(max(drawn.shape))
    beside = index_at[:longest] + [(index_at[longest] + 1) % drawn.shape[longest]] + index_at[longest + 1:]
    return drawn.at[tuple(index_at)].set(low).at[tuple(beside)].set(top_value)


def setup_inputs(seed: int = 0) -> dict:
    key_of = jax.random.split(jax.random.key(seed), 9)
    return {
        "teacher_hidden": draw_teacher_hidden(jax.random.fold_in(key_of[8], 71), 0),
        "student_hidden": draw_student_hidden(jax.random.fold_in(key_of[8], 71), 0),
        "teacher_gain": jnp.clip(1.0 + 0.1 * jax.random.normal(key_of[2], (DT,), jnp.float32), 0.5, 1.5).astype(jnp.bfloat16),
        "student_gain": jnp.clip(1.0 + 0.1 * jax.random.normal(key_of[3], (DS,), jnp.float32), 0.5, 1.5).astype(jnp.bfloat16),
        "teacher_head": draw_teacher_head(jax.random.fold_in(key_of[8], 71), 0),
        "student_head": draw_student_head(jax.random.fold_in(key_of[8], 71), 0),
        "labels": place_ends(jax.random.randint(key_of[6], (TOKENS,), 0, VOCAB), jax.random.fold_in(key_of[6], 1), 0, VOCAB - 1).astype(jnp.int32),
        "cotangent": jnp.clip(jnp.exp(jax.random.uniform(key_of[7], (TOKENS,), jnp.float32, math.log(2.0), math.log(20.0))), 2.0, 20.0),
    }


eps = 1e-06
ce_weight = 0.5

def normalize(hidden, gain):
    values = hidden.astype(jnp.float32)
    inverse = lax.rsqrt(lax.optimization_barrier(jnp.mean(values * values, axis=-1, keepdims=True)) + eps)
    scaled = values * inverse
    return (scaled, inverse, (scaled * gain.astype(jnp.float32)).astype(jnp.bfloat16))

def reference(teacher_hidden, student_hidden, teacher_gain, student_gain, teacher_head, student_head, labels, cotangent):
    _, _, teacher_normed = normalize(teacher_hidden, teacher_gain)
    scaled, inverse, student_normed = normalize(student_hidden, student_gain)
    teacher_logits = lax.dot_general(teacher_normed, teacher_head, (((1,), (1,)), ((), ())), preferred_element_type=jnp.float32)
    student_logits = lax.dot_general(student_normed, student_head, (((1,), (1,)), ((), ())), preferred_element_type=jnp.float32)
    teacher_peak = lax.optimization_barrier(jnp.max(teacher_logits, axis=1, keepdims=True))
    student_peak = lax.optimization_barrier(jnp.max(student_logits, axis=1, keepdims=True))
    teacher_exp = jnp.exp(teacher_logits - teacher_peak)
    teacher_total = lax.optimization_barrier(jnp.sum(teacher_exp, axis=1, keepdims=True))
    cross = lax.optimization_barrier(jnp.sum(teacher_exp * (teacher_logits - student_logits), axis=1, keepdims=True))
    student_total = lax.optimization_barrier(jnp.sum(jnp.exp(student_logits - student_peak), axis=1, keepdims=True))
    columns = lax.broadcasted_iota(jnp.int32, student_logits.shape, 1)
    hits = columns == labels.astype(jnp.int32)[:, None]
    picked = lax.optimization_barrier(jnp.sum(jnp.where(hits, student_logits, 0.0), axis=1, keepdims=True))
    teacher_log = teacher_peak + jnp.log(teacher_total)
    student_log = student_peak + jnp.log(student_total)
    token_loss = cross / teacher_total - teacher_log + student_log + ce_weight * (student_log - picked)
    loss = jnp.mean(token_loss)
    student_prob = jnp.exp(student_logits - student_log)
    teacher_prob = jnp.exp(teacher_logits - teacher_log)
    onehot = jnp.where(hits, 1.0, 0.0).astype(jnp.float32)
    slope = (cotangent[:, None] * ((1.0 + ce_weight) * student_prob - teacher_prob - ce_weight * onehot)).astype(jnp.bfloat16)
    head_grad = lax.dot_general(slope, student_normed, (((0,), (0,)), ((), ())), preferred_element_type=jnp.float32).astype(jnp.bfloat16)
    normed_grad = jnp.dot(slope, student_head, preferred_element_type=jnp.float32)
    gain_grad = lax.optimization_barrier(jnp.sum(normed_grad * scaled, axis=0))
    weighted = normed_grad * student_gain.astype(jnp.float32)
    student_grad = inverse * (weighted - scaled * lax.optimization_barrier(jnp.mean(weighted * scaled, axis=1, keepdims=True)))
    return (loss, student_grad, gain_grad, head_grad)
```

```python
import functools

import jax
import jax.numpy as jnp
from jax import lax
from jax.experimental import pallas as pl
from jax.experimental.pallas import tpu as pltpu
from jax.sharding import PartitionSpec as P

eps = 1e-06
ce_weight = 0.5
f32 = jnp.float32
bf16 = jnp.bfloat16


def copy_to(source, target, sent, landed, section, position):
    return pltpu.make_async_remote_copy(
        src_ref=source,
        dst_ref=target,
        send_sem=sent,
        recv_sem=landed,
        device_id=(section, position),
        device_id_type=pl.DeviceIdType.MESH,
    )


def kernel(
    sections, n,
    th, sh, tg, sg, thead_hbm, shead_hbm, labels, cot,
    loss_out, sgrad_out, gain_out, hgrad_out,
    thead, shead, gt, gs, nt, ns, nsb, scf, tf, hg,
    st1, st2, csend1, crecv1, csend2, cbuf, gacc, esend, ebuf, g1, g2,
    load_sem, out_sem, rt, rs, zt, zs, yt, ys, ct, cs,
    s1s, s1r, s2s, s2r, c1s, c1r, c2s, c2r, es, er, g1s, g1r, g2s, g2r,
):
    S = sections
    A = n // 4
    chips = n // 2
    T = 4 * n
    DS = sh.shape[1]
    Dh = DS // 2
    entries = thead.shape[0]
    s = lax.axis_index("section")
    d = lax.axis_index("dp")
    a, b, c = d // 4, (d // 2) % 2, d % 2
    q = d // 2
    partner = q * 2 + (1 - c)

    def at(a_, b_, c_):
        return (a_ * 2 + b_) * 2 + c_

    across = at(a, 1 - b, c)

    load_t = pltpu.make_async_copy(thead_hbm, thead, load_sem.at[0])
    load_s = pltpu.make_async_copy(shead_hbm, shead, load_sem.at[1])
    load_t.start()
    load_s.start()

    total = S * n
    me = s * n + d
    barrier = pltpu.get_barrier_semaphore()

    def greet(k, carry):
        other = (me + k) % total
        pl.semaphore_signal(
            barrier, inc=1, device_id=(other // n, other % n),
            device_id_type=pl.DeviceIdType.MESH,
        )
        return carry

    lax.fori_loop(1, total, greet, 0)
    pl.semaphore_wait(barrier, total - 1)

    def both(src_t, src_s, slot, sem_t, sem_s, k, position):
        return (
            copy_to(src_s, gs.at[slot], sem_s.at[k], rs.at[slot], s, position),
            copy_to(src_t, gt.at[slot], sem_t.at[k], rt.at[slot], s, position),
        )

    def start(pair):
        for one in pair:
            one.start()

    def landed(slot):
        copy_to(gs.at[slot], gs.at[slot], ys.at[0], rs.at[slot], s, partner).wait_recv()
        copy_to(gt.at[slot], gt.at[slot], yt.at[0], rt.at[slot], s, partner).wait_recv()

    def along(k, carry):
        start(both(th, sh, d, zt, zs, k, at((a + k) % A, b, c)))
        return carry

    lax.fori_loop(1, A, along, 0)
    start(both(th, sh, d, yt, ys, 0, across))
    start(both(th, sh, d, ct, cs, 0, partner))
    gt[d] = th[...]
    gs[d] = sh[...]

    t_gain = tg[...].astype(f32)
    s_gain = sg[...].astype(f32)

    def process(p):
        x = jnp.concatenate([gs[2 * p].astype(f32), gs[2 * p + 1].astype(f32)], axis=0)
        inv = lax.rsqrt(jnp.mean(x * x, axis=1, keepdims=True) + eps)
        scaled = x * inv
        scf[p] = scaled
        ns[p] = scaled * s_gain
        y = jnp.concatenate([gt[2 * p].astype(f32), gt[2 * p + 1].astype(f32)], axis=0)
        inv_t = lax.rsqrt(jnp.mean(y * y, axis=1, keepdims=True) + eps)
        nt[p] = y * inv_t * t_gain

    def near(k, carry):
        slot = at((a - k + A) % A, b, c)
        landed(slot)
        start(both(gt.at[slot], gs.at[slot], slot, yt, ys, k, across))
        start(both(gt.at[slot], gs.at[slot], slot, ct, cs, k, partner))
        before = at((a - k + 1 + A) % A, b, 1 - c)
        landed(before)
        process(before // 2)
        return carry

    lax.fori_loop(1, A, near, 0)

    def far(k, carry):
        slot = at((a - k + A) % A, 1 - b, c)
        landed(slot)
        start(both(gt.at[slot], gs.at[slot], slot, ct, cs, A + k, partner))
        first = jnp.where(k == 0, 1, 0)
        before = at((a - k + 1 + A) % A, jnp.where(first == 1, b, 1 - b), 1 - c)
        landed(before)
        process(before // 2)
        return carry

    lax.fori_loop(0, A, far, 0)
    last = at((a - A + 1 + A) % A, 1 - b, 1 - c)
    landed(last)
    process(last // 2)

    nsb[...] = ns[...].reshape(T, DS).astype(bf16)
    load_s.wait()
    contract = (((1,), (1,)), ((), ()))
    sl = lax.dot_general(shead[...], nsb[...], contract, preferred_element_type=f32)
    load_t.wait()
    tl = lax.dot_general(
        thead[...], nt[...].reshape(T, nt.shape[2]).astype(bf16), contract,
        preferred_element_type=f32,
    )
    rows = lax.broadcasted_iota(jnp.int32, sl.shape, 0) + me * entries
    hits = rows == labels[...]

    tp = jnp.max(tl, axis=0, keepdims=True)
    sp = jnp.max(sl, axis=0, keepdims=True)
    te = jnp.exp(tl - tp)
    own1 = (s * 2 + b) * 2 + c
    stats = (
        tp,
        jnp.sum(te, axis=0, keepdims=True),
        jnp.sum(te * (tl - sl), axis=0, keepdims=True),
        sp,
        jnp.sum(jnp.exp(sl - sp), axis=0, keepdims=True),
        jnp.sum(jnp.where(hits, sl, 0.0), axis=0, keepdims=True),
    )

    def put(ref, slot, values):
        padded = list(values) + [jnp.zeros((8 - len(values), T), f32)]
        ref[slot] = jnp.concatenate(padded, axis=0)

    def merged(ref, count):
        tps = [ref[g, 0:1, :] for g in range(count)]
        sps = [ref[g, 3:4, :] for g in range(count)]
        tp = functools.reduce(jnp.maximum, tps)
        sp = functools.reduce(jnp.maximum, sps)
        tt = cr = stt = pk = 0.0
        for g in range(count):
            w = jnp.exp(tps[g] - tp)
            tt = tt + ref[g, 1:2, :] * w
            cr = cr + ref[g, 2:3, :] * w
            stt = stt + ref[g, 4:5, :] * jnp.exp(sps[g] - sp)
            pk = pk + ref[g, 5:6, :]
        return tp, tt, cr, sp, stt, pk

    def send_all(count, own, ref, sent, got, where):
        def go(k, carry):
            other = (own + k) % count
            copy_to(ref.at[own], ref.at[own], sent.at[k], got.at[own], *where(other)).start()
            return carry

        lax.fori_loop(1, count, go, 0)

    def wait_all(count, own, ref, got):
        def go(k, carry):
            other = (own + k) % count
            copy_to(ref.at[other], ref.at[other], got.at[other], got.at[other], s, partner).wait_recv()
            return carry

        lax.fori_loop(1, count, go, 0)

    def where1(g):
        return g // 4, at(a, (g // 2) % 2, g % 2)

    def where2(g):
        return s, at(g, b, c)

    put(st1, own1, stats)
    send_all(4 * S, own1, st1, s1s, s1r, where1)
    wait_all(4 * S, own1, st1, s1r)
    put(st2, a, merged(st1, 4 * S))
    send_all(A, a, st2, s2s, s2r, where2)
    wait_all(A, a, st2, s2r)
    tp, tt, cr, sp, stt, pk = merged(st2, A)

    t_log = tp + jnp.log(tt)
    s_log = sp + jnp.log(stt)
    token_loss = cr / tt - t_log + s_log + ce_weight * (s_log - pk)
    loss_out[...] = jnp.sum(token_loss, axis=1, keepdims=True) / T
    slope = (
        cot[...]
        * (
            (1.0 + ce_weight) * jnp.exp(sl - s_log)
            - jnp.exp(tl - t_log)
            - ce_weight * jnp.where(hits, 1.0, 0.0)
        )
    ).astype(bf16)

    tf[...] = lax.dot_general(
        slope, shead[...], (((0,), (0,)), ((), ())), preferred_element_type=f32
    ).reshape(chips, 8, DS)
    mine = pl.ds(pl.multiple_of(c * Dh, 128), Dh)
    theirs = pl.ds(pl.multiple_of((1 - c) * Dh, 128), Dh)
    csend1[...] = tf[:, :, theirs].astype(bf16)
    swap = copy_to(csend1, crecv1, c1s, c1r, s, partner)
    swap.start()
    hg[...] = jnp.dot(slope, nsb[...], preferred_element_type=f32).astype(bf16)
    store_h = pltpu.make_async_copy(hg, hgrad_out, out_sem)
    store_h.start()
    swap.wait_recv()

    gacc[...] = jnp.zeros_like(gacc)

    def chip_sum(p):
        block = tf[p, :, mine] + crecv1[p].astype(f32)
        gacc[...] += block * scf[p, :, mine]
        return block

    def scatter(k, carry):
        p = (q + k) % chips
        csend2[p] = chip_sum(p).astype(bf16)
        copy_to(csend2.at[p], cbuf.at[q], c2s.at[k], c2r.at[q], s, p * 2 + c).start()
        return carry

    lax.fori_loop(1, chips, scatter, 0)
    acc = chip_sum(q)

    own_g1 = s * 2 + b
    own_g2 = a * 2 + c
    g1[own_g1] = jnp.sum(gacc[...], axis=0, keepdims=True)
    send_all(2 * S, own_g1, g1, g1s, g1r, lambda g: (g // 2, at(a, g % 2, c)))
    wait_all(2 * S, own_g1, g1, g1r)
    g2[own_g2] = functools.reduce(jnp.add, [g1[g] for g in range(2 * S)])
    send_all(2 * A, own_g2, g2, g2s, g2r, lambda g: (s, at(g // 2, b, g % 2)))

    tf[q, :, mine] = acc

    def gather_sum(k, carry):
        p = (q - k + chips) % chips
        copy_to(cbuf.at[p], cbuf.at[p], c2s.at[0], c2r.at[p], s, partner).wait_recv()
        tf[q, :, mine] += cbuf[p].astype(f32)
        return carry

    lax.fori_loop(1, chips, gather_sum, 0)
    acc = tf[q, :, mine]
    esend[0] = acc[0:4]
    esend[1] = acc[4:8]
    own_e = s * 2 + c
    ebuf[own_e] = esend[c]

    def finish(k, carry):
        other = (own_e + k) % (2 * S)
        copy_to(
            esend.at[other % 2], ebuf.at[own_e], es.at[k], er.at[own_e],
            other // 2, q * 2 + other % 2,
        ).start()
        return carry

    lax.fori_loop(1, 2 * S, finish, 0)
    wait_all(2 * A, own_g2, g2, g2r)
    for h in range(2):
        gain_out[:, h * Dh:(h + 1) * Dh] = functools.reduce(
            jnp.add, [g2[2 * g + h] for g in range(A)]
        )
    x = sh[...].astype(f32)
    inverse = lax.rsqrt(jnp.mean(x * x, axis=1, keepdims=True) + eps)
    wait_all(2 * S, own_e, ebuf, er)
    sums = jnp.zeros((4, 1), f32)
    for h in range(2):
        part = slice(h * Dh, (h + 1) * Dh)
        grad = functools.reduce(jnp.add, [ebuf[2 * g + h] for g in range(S)])
        weighted = grad * s_gain[:, part]
        sgrad_out[:, part] = weighted
        sums = sums + jnp.sum(weighted * (x[:, part] * inverse), axis=1, keepdims=True)
    sgrad_out[...] = inverse * (sgrad_out[...] - (x * inverse) * (sums / DS))

    def sent(ref, sem):
        copy_to(ref, ref, sem, sem, s, partner).wait_send()

    def drain(ref, sems, low, high):
        def go(k, carry):
            sent(ref, sems.at[k])
            return carry

        lax.fori_loop(low, high, go, 0)

    drain(th, zt, 1, A)
    drain(sh, zs, 1, A)
    drain(th, yt, 0, A)
    drain(sh, ys, 0, A)
    drain(th, ct, 0, 2 * A)
    drain(sh, cs, 0, 2 * A)
    drain(st1.at[0], s1s, 1, 4 * S)
    drain(st2.at[0], s2s, 1, A)
    sent(csend1, c1s)
    drain(cbuf.at[0], c2s, 1, chips)
    drain(g1.at[0], g1s, 1, 2 * S)
    drain(g2.at[0], g2s, 1, 2 * A)
    drain(esend.at[0], es, 1, 2 * S)
    store_h.wait()


def on_device(
    sections, n,
    teacher_hidden, student_hidden, teacher_gain, student_gain,
    teacher_head, student_head, labels, cotangent,
):
    S, A, chips = sections, n // 4, n // 2
    T = 4 * n
    rows, DT = teacher_head.shape
    DS = student_head.shape[1]
    Dh = DS // 2
    vmem = pl.BlockSpec(memory_space=pltpu.VMEM)
    anywhere = pl.BlockSpec(memory_space=pl.ANY)
    sem = pltpu.SemaphoreType.DMA
    loss, grad, gain, head = pl.pallas_call(
        functools.partial(kernel, sections, n),
        out_shape=(
            jax.ShapeDtypeStruct((1, 1), f32),
            jax.ShapeDtypeStruct((4, DS), f32),
            jax.ShapeDtypeStruct((1, DS), f32),
            jax.ShapeDtypeStruct((rows, DS), bf16),
        ),
        in_specs=[vmem] * 4 + [anywhere] * 2 + [vmem] * 2,
        out_specs=(vmem, vmem, vmem, anywhere),
        scratch_shapes=[
            pltpu.VMEM((rows, DT), bf16),
            pltpu.VMEM((rows, DS), bf16),
            pltpu.VMEM((n, 4, DT), bf16),
            pltpu.VMEM((n, 4, DS), bf16),
            pltpu.VMEM((chips, 8, DT), f32),
            pltpu.VMEM((chips, 8, DS), f32),
            pltpu.VMEM((T, DS), bf16),
            pltpu.VMEM((chips, 8, DS), f32),
            pltpu.VMEM((chips, 8, DS), f32),
            pltpu.VMEM((rows, DS), bf16),
            pltpu.VMEM((4 * S, 8, T), f32),
            pltpu.VMEM((A, 8, T), f32),
            pltpu.VMEM((chips, 8, Dh), bf16),
            pltpu.VMEM((chips, 8, Dh), bf16),
            pltpu.VMEM((chips, 8, Dh), bf16),
            pltpu.VMEM((chips, 8, Dh), bf16),
            pltpu.VMEM((8, Dh), f32),
            pltpu.VMEM((2, 4, Dh), f32),
            pltpu.VMEM((2 * S, 4, Dh), f32),
            pltpu.VMEM((2 * S, 1, Dh), f32),
            pltpu.VMEM((2 * A, 1, Dh), f32),
            sem((2,)), sem,
            sem((n,)), sem((n,)),
            sem((A,)), sem((A,)), sem((A,)), sem((A,)), sem((2 * A,)), sem((2 * A,)),
            sem((4 * S,)), sem((4 * S,)), sem((A,)), sem((A,)),
            sem, sem, sem((chips,)), sem((chips,)),
            sem((2 * S,)), sem((2 * S,)), sem((2 * S,)), sem((2 * S,)),
            sem((2 * A,)), sem((2 * A,)),
        ],
        compiler_params=pltpu.CompilerParams(
            collective_id=0, has_side_effects=True, vmem_limit_bytes=60 * 1024 * 1024
        ),
        name="distill",
    )(
        teacher_hidden, student_hidden,
        teacher_gain.reshape(1, DT), student_gain.reshape(1, DS),
        teacher_head, student_head,
        labels.reshape(1, T), cotangent.reshape(1, T),
    )
    return loss[0, 0], grad, gain[0], head


def solution(mesh):
    return jax.shard_map(
        functools.partial(on_device, mesh.shape["section"], mesh.shape["dp"]),
        mesh=mesh,
        in_specs=(
            P("dp", None),
            P("dp", None),
            P(),
            P(),
            P(("section", "dp"), None),
            P(("section", "dp"), None),
            P(),
            P(),
        ),
        out_specs=(P(), P("dp", None), P(), P(("section", "dp"), None)),
        check_vma=False,
    )
```

```python
import functools

import jax
import jax.numpy as jnp
from jax import lax
from jax.experimental import pallas as pl
from jax.experimental.pallas import tpu as pltpu
from jax.sharding import PartitionSpec as P

eps = 1e-06
ce_weight = 0.5
f32 = jnp.float32
bf16 = jnp.bfloat16


def copy_to(source, target, sent, landed, section, position):
    return pltpu.make_async_remote_copy(
        src_ref=source,
        dst_ref=target,
        send_sem=sent,
        recv_sem=landed,
        device_id=(section, position),
        device_id_type=pl.DeviceIdType.MESH,
    )


def kernel(
    sections, n,
    th_hbm, sh_hbm, tg_hbm, sg_hbm, thead_hbm, shead_hbm, labels_hbm, cot_hbm,
    loss_out, sgrad_out, gain_out, slope_out, nsb_out,
    thead, shead, th, sh, tg, sg, labels, cot, tgr, sgr, gt, gs, nt, ns, nsb, scf, tf,
    st1, st2, csend1, crecv1, csend2, cbuf, gacc, esend, ebuf, g1, g2,
    load_sem, out_sem, in_sem, rt, rs, zt, zs, yt, ys, ct, cs,
    s1s, s1r, s2s, s2r, c1s, c1r, c2s, c2r, es, er, g1s, g1r, g2s, g2r,
):
    S = sections
    A = n // 4
    chips = n // 2
    R = th.shape[0]
    T = R * n
    DS = sh.shape[1]
    Dh = DS // 2
    entries = thead.shape[0]
    s = lax.axis_index("section")
    d = lax.axis_index("dp")
    a, b, c = d // 4, (d // 2) % 2, d % 2
    q = d // 2
    partner = q * 2 + (1 - c)

    def at(a_, b_, c_):
        return (a_ * 2 + b_) * 2 + c_

    across = at(a, 1 - b, c)

    small = [
        pltpu.make_async_copy(source, target, in_sem.at[i])
        for i, (source, target) in enumerate(
            ((th_hbm, th), (sh_hbm, sh), (tg_hbm, tg), (sg_hbm, sg), (labels_hbm, labels), (cot_hbm, cot))
        )
    ]
    load_t = pltpu.make_async_copy(thead_hbm, thead, load_sem.at[0])
    load_s = pltpu.make_async_copy(shead_hbm, shead, load_sem.at[1])

    total = S * n
    me = s * n + d
    barrier = pltpu.get_barrier_semaphore()

    def greet(k, carry):
        other = (me + k) % total
        pl.semaphore_signal(
            barrier, inc=1, device_id=(other // n, other % n),
            device_id_type=pl.DeviceIdType.MESH,
        )
        return carry

    lax.fori_loop(1, total, greet, 0)
    for one in small:
        one.start()
    load_s.start()
    load_t.start()
    for one in small:
        one.wait()
    pl.semaphore_wait(barrier, total - 1)

    def both(src_t, src_s, slot, sem_t, sem_s, k, position):
        return (
            copy_to(src_s, gs.at[slot], sem_s.at[k], rs.at[slot], s, position),
            copy_to(src_t, gt.at[slot], sem_t.at[k], rt.at[slot], s, position),
        )

    def start(pair):
        for one in pair:
            one.start()

    def landed(slot):
        copy_to(gs.at[slot], gs.at[slot], ys.at[0], rs.at[slot], s, partner).wait_recv()
        copy_to(gt.at[slot], gt.at[slot], yt.at[0], rt.at[slot], s, partner).wait_recv()

    def along(k, carry):
        start(both(th, sh, d, zt, zs, k, at((a + k) % A, b, c)))
        return carry

    lax.fori_loop(1, A, along, 0)
    start(both(th, sh, d, yt, ys, 0, across))
    start(both(th, sh, d, ct, cs, 0, partner))
    gt[d] = th[...]
    gs[d] = sh[...]

    for source, target in ((tg, tgr), (sg, sgr)):
        values = source[...].astype(f32)
        for i in range(source.shape[0]):
            target[:, i * 128:(i + 1) * 128] = values[i:i + 1, :]
    s_gain = sgr[...]

    def process(p):
        x = jnp.concatenate([gs[2 * p].astype(f32), gs[2 * p + 1].astype(f32)], axis=0)
        inv = lax.rsqrt(jnp.mean(x * x, axis=1, keepdims=True) + eps)
        scaled = x * inv
        scf[p] = scaled
        ns[p] = scaled * sgr[...]
        y = jnp.concatenate([gt[2 * p].astype(f32), gt[2 * p + 1].astype(f32)], axis=0)
        inv_t = lax.rsqrt(jnp.mean(y * y, axis=1, keepdims=True) + eps)
        nt[p] = y * inv_t * tgr[...]

    def near(k, carry):
        slot = at((a - k + A) % A, b, c)
        landed(slot)
        start(both(gt.at[slot], gs.at[slot], slot, yt, ys, k, across))
        start(both(gt.at[slot], gs.at[slot], slot, ct, cs, k, partner))
        before = at((a - k + 1 + A) % A, b, 1 - c)
        landed(before)
        process(before // 2)
        return carry

    lax.fori_loop(1, A, near, 0)

    def far(k, carry):
        slot = at((a - k + A) % A, 1 - b, c)
        landed(slot)
        start(both(gt.at[slot], gs.at[slot], slot, ct, cs, A + k, partner))
        first = jnp.where(k == 0, 1, 0)
        before = at((a - k + 1 + A) % A, jnp.where(first == 1, b, 1 - b), 1 - c)
        landed(before)
        process(before // 2)
        return carry

    lax.fori_loop(0, A, far, 0)
    last = at((a - A + 1 + A) % A, 1 - b, 1 - c)
    landed(last)
    process(last // 2)

    nsb[...] = ns[...].reshape(T, DS).astype(bf16)
    load_s.wait()
    contract = (((1,), (1,)), ((), ()))
    sl = lax.dot_general(shead[...], nsb[...], contract, preferred_element_type=f32)
    load_t.wait()
    tl = lax.dot_general(
        thead[...], nt[...].reshape(T, nt.shape[2]).astype(bf16), contract,
        preferred_element_type=f32,
    )
    rows = lax.broadcasted_iota(jnp.int32, sl.shape, 0) + me * entries
    hits = rows == labels[...]

    tp = jnp.max(tl, axis=0, keepdims=True)
    sp = jnp.max(sl, axis=0, keepdims=True)
    te = jnp.exp(tl - tp)
    own1 = (s * 2 + b) * 2 + c
    stats = (
        tp,
        jnp.sum(te, axis=0, keepdims=True),
        jnp.sum(te * (tl - sl), axis=0, keepdims=True),
        sp,
        jnp.sum(jnp.exp(sl - sp), axis=0, keepdims=True),
        jnp.sum(jnp.where(hits, sl, 0.0), axis=0, keepdims=True),
    )

    def put(ref, slot, values):
        padded = list(values) + [jnp.zeros((8 - len(values), T), f32)]
        ref[slot] = jnp.concatenate(padded, axis=0)

    def merged(ref, count):
        tps = [ref[g, 0:1, :] for g in range(count)]
        sps = [ref[g, 3:4, :] for g in range(count)]
        tp = functools.reduce(jnp.maximum, tps)
        sp = functools.reduce(jnp.maximum, sps)
        tt = cr = stt = pk = 0.0
        for g in range(count):
            w = jnp.exp(tps[g] - tp)
            tt = tt + ref[g, 1:2, :] * w
            cr = cr + ref[g, 2:3, :] * w
            stt = stt + ref[g, 4:5, :] * jnp.exp(sps[g] - sp)
            pk = pk + ref[g, 5:6, :]
        return tp, tt, cr, sp, stt, pk

    def send_all(count, own, ref, sent, got, where):
        def go(k, carry):
            other = (own + k) % count
            copy_to(ref.at[own], ref.at[own], sent.at[k], got.at[own], *where(other)).start()
            return carry

        lax.fori_loop(1, count, go, 0)

    def wait_all(count, own, ref, got):
        def go(k, carry):
            other = (own + k) % count
            copy_to(ref.at[other], ref.at[other], got.at[other], got.at[other], s, partner).wait_recv()
            return carry

        lax.fori_loop(1, count, go, 0)

    def where1(g):
        return g // 4, at(a, (g // 2) % 2, g % 2)

    def where2(g):
        return s, at(g, b, c)

    put(st1, own1, stats)
    send_all(4 * S, own1, st1, s1s, s1r, where1)
    wait_all(4 * S, own1, st1, s1r)
    put(st2, a, merged(st1, 4 * S))
    send_all(A, a, st2, s2s, s2r, where2)
    wait_all(A, a, st2, s2r)
    tp, tt, cr, sp, stt, pk = merged(st2, A)

    t_log = tp + jnp.log(tt)
    s_log = sp + jnp.log(stt)
    token_loss = cr / tt - t_log + s_log + ce_weight * (s_log - pk)
    loss_out[...] = jnp.sum(token_loss, axis=1, keepdims=True) / T
    slope = (
        cot[...]
        * (
            (1.0 + ce_weight) * jnp.exp(sl - s_log)
            - jnp.exp(tl - t_log)
            - ce_weight * jnp.where(hits, 1.0, 0.0)
        )
    ).astype(bf16)

    tf[...] = lax.dot_general(
        slope, shead[...], (((0,), (0,)), ((), ())), preferred_element_type=f32
    ).reshape(chips, 2 * R, DS)
    mine = pl.ds(pl.multiple_of(c * Dh, 128), Dh)
    theirs = pl.ds(pl.multiple_of((1 - c) * Dh, 128), Dh)
    csend1[...] = tf[:, :, theirs].astype(bf16)
    swap = copy_to(csend1, crecv1, c1s, c1r, s, partner)
    swap.start()
    slope_out[...] = slope
    store_n = pltpu.make_async_copy(nsb, nsb_out, out_sem)
    store_n.start()
    swap.wait_recv()

    gacc[...] = jnp.zeros_like(gacc)

    def chip_sum(p):
        block = tf[p, :, mine] + crecv1[p].astype(f32)
        gacc[...] += block * scf[p, :, mine]
        return block

    def scatter(k, carry):
        p = (q + k) % chips
        csend2[p] = chip_sum(p).astype(bf16)
        copy_to(csend2.at[p], cbuf.at[q], c2s.at[k], c2r.at[q], s, p * 2 + c).start()
        return carry

    lax.fori_loop(1, chips, scatter, 0)
    acc = chip_sum(q)

    own_g1 = s * 2 + b
    own_g2 = a * 2 + c
    g1[own_g1] = jnp.sum(gacc[...], axis=0, keepdims=True)
    send_all(2 * S, own_g1, g1, g1s, g1r, lambda g: (g // 2, at(a, g % 2, c)))
    wait_all(2 * S, own_g1, g1, g1r)
    g2[own_g2] = functools.reduce(jnp.add, [g1[g] for g in range(2 * S)])
    send_all(2 * A, own_g2, g2, g2s, g2r, lambda g: (s, at(g // 2, b, g % 2)))

    tf[q, :, mine] = acc

    def gather_sum(k, carry):
        p = (q - k + chips) % chips
        copy_to(cbuf.at[p], cbuf.at[p], c2s.at[0], c2r.at[p], s, partner).wait_recv()
        tf[q, :, mine] += cbuf[p].astype(f32)
        return carry

    lax.fori_loop(1, chips, gather_sum, 0)
    acc = tf[q, :, mine]
    esend[0] = acc[0:R]
    esend[1] = acc[R:2 * R]
    own_e = s * 2 + c
    ebuf[own_e] = esend[c]

    def finish(k, carry):
        other = (own_e + k) % (2 * S)
        copy_to(
            esend.at[other % 2], ebuf.at[own_e], es.at[k], er.at[own_e],
            other // 2, q * 2 + other % 2,
        ).start()
        return carry

    lax.fori_loop(1, 2 * S, finish, 0)
    wait_all(2 * A, own_g2, g2, g2r)
    for h in range(2):
        gain_out[:, h * Dh:(h + 1) * Dh] = functools.reduce(
            jnp.add, [g2[2 * g + h] for g in range(A)]
        )
    x = sh[...].astype(f32)
    inverse = lax.rsqrt(jnp.mean(x * x, axis=1, keepdims=True) + eps)
    wait_all(2 * S, own_e, ebuf, er)
    sums = jnp.zeros((R, 1), f32)
    for h in range(2):
        part = slice(h * Dh, (h + 1) * Dh)
        grad = functools.reduce(jnp.add, [ebuf[2 * g + h] for g in range(S)])
        weighted = grad * s_gain[:, part]
        sgrad_out[:, part] = weighted
        sums = sums + jnp.sum(weighted * (x[:, part] * inverse), axis=1, keepdims=True)
    sgrad_out[...] = inverse * (sgrad_out[...] - (x * inverse) * (sums / DS))

    def sent(ref, sem):
        copy_to(ref, ref, sem, sem, s, partner).wait_send()

    def drain(ref, sems, low, high):
        def go(k, carry):
            sent(ref, sems.at[k])
            return carry

        lax.fori_loop(low, high, go, 0)

    drain(th, zt, 1, A)
    drain(sh, zs, 1, A)
    drain(th, yt, 0, A)
    drain(sh, ys, 0, A)
    drain(th, ct, 0, 2 * A)
    drain(sh, cs, 0, 2 * A)
    drain(st1.at[0], s1s, 1, 4 * S)
    drain(st2.at[0], s2s, 1, A)
    sent(csend1, c1s)
    drain(cbuf.at[0], c2s, 1, chips)
    drain(g1.at[0], g1s, 1, 2 * S)
    drain(g2.at[0], g2s, 1, 2 * A)
    drain(esend.at[0], es, 1, 2 * S)
    store_n.wait()


def finish_kernel(slope, normed, loss, grad, gain, loss_out, grad_out, gain_out, head_out):
    head_out[...] = jnp.dot(slope[...], normed[...], preferred_element_type=f32).astype(bf16)
    loss_out[...] = loss[...]
    grad_out[...] = grad[...]
    for i in range(gain_out.shape[0]):
        gain_out[i:i + 1, :] = gain[:, i * 128:(i + 1) * 128]


def on_device(
    sections, n,
    teacher_hidden, student_hidden, teacher_gain, student_gain,
    teacher_head, student_head, labels, cotangent,
):
    S, A, chips = sections, n // 4, n // 2
    R = teacher_hidden.shape[0]
    T = R * n
    rows, DT = teacher_head.shape
    DS = student_head.shape[1]
    Dh = DS // 2
    vmem = pl.BlockSpec(memory_space=pltpu.VMEM)
    anywhere = pl.BlockSpec(memory_space=pl.ANY)
    sem = pltpu.SemaphoreType.DMA
    loss, grad, gain, slope, normed = pl.pallas_call(
        functools.partial(kernel, sections, n),
        out_shape=(
            jax.ShapeDtypeStruct((1, 1), f32),
            jax.ShapeDtypeStruct((R, DS), f32),
            jax.ShapeDtypeStruct((1, DS), f32),
            jax.ShapeDtypeStruct((rows, T), bf16),
            jax.ShapeDtypeStruct((T, DS), bf16),
        ),
        in_specs=[anywhere] * 8,
        out_specs=(vmem, vmem, vmem, vmem, anywhere),
        scratch_shapes=[
            pltpu.VMEM((rows, DT), bf16),
            pltpu.VMEM((rows, DS), bf16),
            pltpu.VMEM((R, DT), bf16),
            pltpu.VMEM((R, DS), bf16),
            pltpu.VMEM((DT // 128, 128), bf16),
            pltpu.VMEM((DS // 128, 128), bf16),
            pltpu.VMEM((1, T), jnp.int32),
            pltpu.VMEM((1, T), f32),
            pltpu.VMEM((1, DT), f32),
            pltpu.VMEM((1, DS), f32),
            pltpu.VMEM((n, R, DT), bf16),
            pltpu.VMEM((n, R, DS), bf16),
            pltpu.VMEM((chips, 2 * R, DT), f32),
            pltpu.VMEM((chips, 2 * R, DS), f32),
            pltpu.VMEM((T, DS), bf16),
            pltpu.VMEM((chips, 2 * R, DS), f32),
            pltpu.VMEM((chips, 2 * R, DS), f32),
            pltpu.VMEM((4 * S, 8, T), f32),
            pltpu.VMEM((A, 8, T), f32),
            pltpu.VMEM((chips, 2 * R, Dh), bf16),
            pltpu.VMEM((chips, 2 * R, Dh), bf16),
            pltpu.VMEM((chips, 2 * R, Dh), bf16),
            pltpu.VMEM((chips, 2 * R, Dh), bf16),
            pltpu.VMEM((2 * R, Dh), f32),
            pltpu.VMEM((2, R, Dh), f32),
            pltpu.VMEM((2 * S, R, Dh), f32),
            pltpu.VMEM((2 * S, 1, Dh), f32),
            pltpu.VMEM((2 * A, 1, Dh), f32),
            sem((2,)), sem, sem((6,)),
            sem((n,)), sem((n,)),
            sem((A,)), sem((A,)), sem((A,)), sem((A,)), sem((2 * A,)), sem((2 * A,)),
            sem((4 * S,)), sem((4 * S,)), sem((A,)), sem((A,)),
            sem, sem, sem((chips,)), sem((chips,)),
            sem((2 * S,)), sem((2 * S,)), sem((2 * S,)), sem((2 * S,)),
            sem((2 * A,)), sem((2 * A,)),
        ],
        compiler_params=pltpu.CompilerParams(
            collective_id=0, has_side_effects=True, vmem_limit_bytes=60 * 1024 * 1024
        ),
        name="distill",
    )(
        teacher_hidden, student_hidden,
        teacher_gain.reshape(DT // 128, 128), student_gain.reshape(DS // 128, 128),
        teacher_head, student_head,
        labels.reshape(1, T), cotangent.reshape(1, T),
    )
    steps = 4
    width = DS // steps

    def whole(*shape):
        return pl.BlockSpec(shape, lambda i: (0, 0))

    loss, grad, gain, head = pl.pallas_call(
        finish_kernel,
        grid=(steps,),
        out_shape=(
            jax.ShapeDtypeStruct((1, 1), f32),
            jax.ShapeDtypeStruct((R, DS), f32),
            jax.ShapeDtypeStruct((DS // 128, 128), f32),
            jax.ShapeDtypeStruct((rows, DS), bf16),
        ),
        in_specs=[
            whole(rows, T), pl.BlockSpec((T, width), lambda i: (0, i)),
            whole(1, 1), whole(R, DS), whole(1, DS),
        ],
        out_specs=(
            whole(1, 1), whole(R, DS), whole(DS // 128, 128),
            pl.BlockSpec((rows, width), lambda i: (0, i)),
        ),
        name="head",
    )(slope, normed, loss, grad, gain)
    return loss[0, 0], grad, gain.reshape(DS), head


def solution(mesh):
    return jax.shard_map(
        functools.partial(on_device, mesh.shape["section"], mesh.shape["dp"]),
        mesh=mesh,
        in_specs=(
            P("dp", None),
            P("dp", None),
            P(),
            P(),
            P(("section", "dp"), None),
            P(("section", "dp"), None),
            P(),
            P(),
        ),
        out_specs=(P(), P("dp", None), P(), P(("section", "dp"), None)),
        check_vma=False,
    )
```
